32 devices in a mesh: row: 8 (over y, x, core), col: 4 (over z).
Axes of the slice: x: 2, y: 2, z: 4, core: 2. Of those that a mesh axis runs over, the one named last changes fastest.
Arguments:
- vectors: float32 [16384, 16384], P('row', 'col'), may hold values from -0.046875 to 0.046875
- basis: float32 [16384, 2048], P('col', 'row'), may hold values from -9 to 9
- block_units: int32 [8], replicated, may hold values from 1 to 40, 64 in all
Outputs:
- assembled: float32 [16384, 2048], P('row', 'col')
The draws below stay inside these ranges and needn't reach their ends.
Inputs may be any that keep to these rules, and one draw needn't show every extreme that they name: `block_units`: the block sizes are whole numbers of units that sum to 64; the largest is exactly the maximum.
All inputs are finite; a program needn't handle non-finite values.
Results may differ from the reference program's by a relative error of at most 0.00007.
Values sent between devices are 32-bit elements; how exact they have to be, the bound alone decides.
A program may use at most 192 MiB of HBM per device.

```python
import math
import jax
import jax.numpy as jnp
import numpy as np
from jax import lax

N = 16384
W = 2048
UNIT = 256
BLOCKS = 8
START = 7168


def block_scale(own_key, extent, cuts, smallest, largest):
    def one(axis_at, shards_of):
        heights = jax.random.uniform(jax.random.fold_in(jax.random.fold_in(own_key, 6), axis_at), (shards_of,), jnp.float32, smallest / len(cuts), largest / len(cuts))
        return jnp.repeat(jnp.exp(heights), extent[axis_at] // shards_of).reshape((-1,) + (1,) * (len(extent) - axis_at - 1))

    level = one(*cuts[0])
    for cut in cuts[1:]:
        level = level * one(*cut)
    return level


def length_profile(count, total, reach, skew):
    weights = [(1 << 20) // math.isqrt(standing ** skew) + 1 for standing in range(2, count + 1)]
    surplus, counts = total - reach - (count - 1), [1] * (count - 1)
    while surplus > 0:
        candidates = [i for i in range(count - 1) if counts[i] < reach]
        mass, left = sum([weights[i] for i in candidates]), surplus
        for i in candidates:
            extra = min(reach - counts[i], max(1, left * weights[i] // mass), surplus)
            counts[i] = counts[i] + extra
            surplus = surplus - extra
    return np.array([reach] + counts)


def uneven_parts(key, amount, total, most, slope):
    if amount == 2:
        one = jax.random.randint(key, (), max(1, total - most), min(most, total - 1) + 1)
        return jnp.stack([one, total - one])
    tallies = jnp.asarray(length_profile(amount, total, most, slope), jnp.int32)
    couples = (amount - 1) // 2
    donor, receiver = tallies[1:1 + 2 * couples:2], tallies[2:2 + 2 * couples:2]
    room = jnp.minimum(donor - 1, most - receiver)
    moved = jax.random.randint(jax.random.fold_in(key, 1), (couples,), 0, 1 << 20) % (room + 1)
    tallies = tallies.at[1:1 + 2 * couples:2].set(donor - moved).at[2:2 + 2 * couples:2].set(receiver + moved)
    return tallies[jax.random.permutation(jax.random.fold_in(key, 2), amount)]


def bell_draw(own_key, dims, spread, bound, pieces=(), held_as=jnp.bfloat16):
    array = spread * jax.random.normal(own_key, dims, jnp.float32)
    if pieces:
        array = array * block_scale(own_key, dims, pieces, -0.22, 0.18)
    return jnp.clip(array, -bound, bound).astype(held_as)


def setup_inputs(seed: int = 0) -> dict:
    key_list = jax.random.split(jax.random.key(seed), 4)
    return {
        "vectors": bell_draw(key_list[0], (N, N), N ** -0.5, 0.046875, ((0, 8), (1, 4)), jnp.float32),
        "basis": bell_draw(key_list[1], (N, W), 1.5, 9.0, ((0, 4), (1, 8)), jnp.float32),
        "block_units": uneven_parts(key_list[2], BLOCKS, N // UNIT, 5 * N // (8 * UNIT), 2).astype(jnp.int32),
    }


def block_ids(positions, block_units):
    ends = jnp.cumsum(block_units).astype(jnp.int32) * UNIT
    return jnp.sum((positions[:, None] >= ends[None, :-1]).astype(jnp.int32), axis=1)


def reference(vectors, basis, block_units):
    row_block = block_ids(jnp.arange(N, dtype=jnp.int32), block_units)
    slab_block = block_ids(START + jnp.arange(W, dtype=jnp.int32), block_units)
    masked = jnp.where(row_block[:, None] == slab_block[None, :], basis, jnp.float32(0.0))
    return jnp.dot(vectors, masked, precision=lax.Precision.HIGHEST, preferred_element_type=jnp.float32)
```

```python
import jax
import jax.numpy as jnp
from jax import lax
from jax.sharding import PartitionSpec as P

UNIT = 256
START = 7168
LANES = 128


def block_ids(positions, block_units):
    ends = jnp.cumsum(block_units) * UNIT
    return jnp.sum((positions[:, None] >= ends[None, :-1]).astype(jnp.int32), axis=1)


def shards(vectors, basis, block_units):
    inner, width = basis.shape
    row_block = block_ids(
        lax.axis_index("col") * inner + jnp.arange(inner, dtype=jnp.int32), block_units
    )
    slab_block = block_ids(
        START + lax.axis_index("row") * width + jnp.arange(width, dtype=jnp.int32), block_units
    )
    masked = jnp.where(row_block[:, None] == slab_block[None, :], basis, jnp.float32(0.0))

    rows, cols = lax.axis_size("row"), lax.axis_size("col")
    step = LANES if width % LANES == 0 and rows % cols == 0 else width
    pieces = [
        lax.all_gather(masked[:, at:at + step], "row", axis=1, tiled=True)
        for at in range(0, width, step)
    ]
    sums = []
    for piece in pieces:
        part = jnp.dot(
            vectors, piece, precision=lax.Precision.HIGH, preferred_element_type=jnp.float32
        )
        sums.append(lax.psum_scatter(part, "col", scatter_dimension=1, tiled=True))
    groups = sums[0].shape[1] // step
    return jnp.concatenate(
        [one[:, g * step:(g + 1) * step] for g in range(groups) for one in sums], axis=1
    )


def solution(mesh):
    in_specs = (P("row", "col"), P("col", "row"), P())
    out_specs = P("row", "col")
    return jax.shard_map(shards, mesh=mesh, in_specs=in_specs, out_specs=out_specs, check_vma=False)
```
